32 devices in a mesh: fluid: 8 (over z, x), solid: 4 (over y, core).
Axes of the slice: x: 2, y: 2, z: 4, core: 2. Of those that a mesh axis runs over, the one named last changes fastest.
Arguments:
- flow: bfloat16 [3, 262144, 128], P(None, ('fluid', 'solid')), may hold values from -6 to 6
- wall_motion: float32 [3, 262144], P(None, ('fluid', 'solid')), may hold values from -6 to 6
- normal_operator: bfloat16 [128, 128], replicated, may hold values from -0.5 to 0.5
- wall_coupling: float32 [128], replicated, may hold values from -4 to 4
- wall_stencil: bfloat16 [128], replicated, may hold values from -0.5 to 0.5
- rbf_blocks: bfloat16 [2048, 128, 128], P(('fluid', 'solid')), may hold values from -0.5 to 0.5
- block_owner: int32 [2048, 1], P(('fluid', 'solid')), may hold values from 0 to 7; in each aligned block of 64 rows (0 to 63, 64 to 127, ...) at most 12 rows name the same one
- block_row: int32 [2048, 1], P(('fluid', 'solid')), may hold values from 0 to 31
- displacement: float32 [1024, 3, 128], P(('fluid', 'solid')), may hold values from -6 to 6
- stiffness: float32 [1024, 128], P(('fluid', 'solid')), may hold values from 0.5 to 4
- residual_history: float32 [64, 1024, 3, 128], P(None, ('fluid', 'solid')), may hold values from -0.076546554 to 0.076546554
- solution_history: float32 [64, 1024, 3, 128], P(None, ('fluid', 'solid')), may hold values from -6 to 6
Outputs:
- new_flow: bfloat16 [3, 262144, 128], P(None, ('fluid', 'solid'))
- next_displacement: float32 [1024, 3, 128], P(('fluid', 'solid'))
- wall_next: float32 [3, 262144], P(None, ('fluid', 'solid'))
- residual_norm: float32 [], replicated
The draws below stay inside these ranges and needn't reach their ends.
Inputs may be any that keep to these rules, and one draw needn't show every extreme that they name: `block_owner`: each device's 64 blocks name no owner more than 12 times, a bound that some block reaches; every owner gets some block.
All inputs are finite; a program needn't handle non-finite values.
Results may differ from the reference program's by a relative error of at most 0.0035.
The reference program's roundings to bfloat16 on the way (of `traction`) count: a program that leaves them out, or rounds other values in their place, can miss the bound.
Values may be sent and summed in bfloat16 or wider, within the bound.
No kernel may reach another device: no remote copies, remote signals or barrier semaphores. Data moves between devices by JAX's collectives and lax.ppermute only.
A program may use at most 128 MiB of HBM per device.

```python
import math
import jax
import jax.numpy as jnp
import numpy as np
from jax import lax

NW = 128
BLOCK = 128
SW = 128
HIST = 64
SWEEPS = 4
SR = 32
FB = 64
MOST = 12
NS = 262144
FBLOCKS = 2048
NSR = 1024
N_FLUID = 8
N_SOLID = 4


def draw_residual_history(key, part):
    entries = NSR * 3 * SW
    subkeys = jax.random.split(jax.random.fold_in(key, 71), 4)
    directions = 4
    private = jax.random.normal(subkeys[0], (HIST, entries), jnp.float32)
    weights = 0.5 ** jnp.arange(directions, dtype=jnp.float32)
    shared = jax.random.normal(subkeys[2], (directions, entries), jnp.float32)
    mixing = jax.random.normal(subkeys[3], (HIST, directions), jnp.float32) * weights[None, :]
    common = jnp.dot(mixing, shared, precision=lax.Precision.HIGHEST)
    magnitude = math.sqrt(HIST / entries)
    values = jnp.clip(magnitude * (private + common), -6.0 * magnitude, 6.0 * magnitude)
    return values.astype(jnp.float32).reshape(HIST, NSR, 3, SW)


def touch_ends(values, stream_key, smallest, high):
    longest = values.shape.index(max(values.shape))
    spots = []
    for shift in (0, 1):
        where = [jax.random.randint(jax.random.fold_in(stream_key, axis), (), 0, length) for axis, length in enumerate(values.shape)]
        where[longest] = (where[longest] + shift) % values.shape[longest]
        spots.append(tuple(where))
    return values.at[spots[0]].set(smallest).at[spots[1]].set(high)


def level_of(rng, extent, cuts, smallest, largest):
    level, own = 1.0, jax.random.fold_in(rng, 6)
    for dim, shards_of in cuts:
        steps = jnp.exp(jax.random.uniform(jax.random.fold_in(own, dim), (shards_of,), jnp.float32, smallest / len(cuts), largest / len(cuts)))
        level = level * jnp.repeat(steps, extent[dim] // shards_of).reshape([-1 if axis == dim else 1 for axis in range(len(extent))])
    return level


def deal_out(key, own, number, rows, number_of, top, bound, skew):
    order = jax.random.permutation(key, number_of)
    packed, usual = portions_of(number_of, rows * top, bound, skew, True), portions_of(number_of, rows * top, bound, skew, False)
    places = jnp.arange(number_of)

    def named(lengths, turn):
        used = int((lengths > 0).sum())
        fixed = max(1, used // 4)
        passed = fixed + (places - fixed + turn * (used - fixed)) % max(1, number_of - fixed)
        return jnp.zeros((number_of,), jnp.int32).at[order[jnp.where(places < fixed, places, passed)]].set(jnp.asarray(lengths, jnp.int32))

    lengths = jnp.where(number % 4 == 0, named(packed, number // 4), named(usual, number - number // 4 - 1))
    mixed = jax.random.permutation(jax.random.fold_in(own, 3), number_of)
    source_of, sink = mixed[0:number_of // 2 * 2:2], mixed[1:number_of // 2 * 2:2]
    room = jnp.minimum(lengths[source_of] - 1, bound - lengths[sink]) // 2
    room = jnp.where((source_of == order[0]) | (sink == order[0]) | (lengths[sink] == 0), 0, jnp.maximum(room, 0))
    passed = jax.random.randint(jax.random.fold_in(own, 4), (number_of // 2,), 0, 1 << 20) % (room + 1)
    lengths = lengths.at[source_of].add(-passed).at[sink].add(passed)
    members = jnp.searchsorted(jnp.cumsum(lengths), jnp.arange(rows * top), side="right").astype(jnp.int32)
    table = members.reshape(top, rows).T
    table = table[jax.random.permutation(jax.random.fold_in(own, 1), rows)]
    turn = jax.random.randint(jax.random.fold_in(own, 2), (rows, 1), 0, top)
    return jnp.take_along_axis(table, (jnp.arange(top)[None, :] + turn) % top, axis=1)


def portions_of(number_of, total, bound, skew, full):
    portions = [(1 << 20) // math.isqrt(rank ** skew) + 1 for rank in range(1, number_of + 1)]
    largest = bound if full else min(bound, max(-(-total // number_of), total * portions[0] // sum(portions)))
    least = 1 if total - largest >= number_of - 1 else 0
    holding, surplus = [largest] + [least] * (number_of - 1), total - largest - least * (number_of - 1)
    while surplus > 0:
        free = [i for i in range(1, number_of) if holding[i] < largest] or [i for i in range(1, number_of) if holding[i] < bound]
        pool, remaining = sum([portions[i] for i in free]), surplus
        for i in free:
            addition = min(bound - holding[i], max(1, remaining * portions[i] // pool), surplus)
            holding[i] = holding[i] + addition
            surplus = surplus - addition
    return np.array(holding)


def bell_draw(stream_key, dims, deviation, most, shards=(), held_as=jnp.bfloat16):
    result = jax.random.normal(stream_key, dims, jnp.float32) * deviation
    if len(shards) > 0:
        result = level_of(stream_key, dims, shards, -0.22, 0.18) * result
    return jnp.clip(result, min=-most, max=most).astype(held_as)


def setup_inputs(seed: int = 0) -> dict:
    splits = jax.random.split(jax.random.key(seed), 13)
    flow = bell_draw(splits[0], (3, NS, NW), 1.0, 6.0, ((1, 32),))
    wall_motion = bell_draw(splits[1], (3, NS), 1.0, 6.0, ((1, 32),), jnp.float32)
    normal_operator = bell_draw(splits[2], (NW, NW), NW ** -0.5, 0.5)
    wall_coupling = bell_draw(splits[3], (NW,), 1.0, 4.0, (), jnp.float32)
    wall_stencil = bell_draw(splits[4], (NW,), NW ** -0.5, 0.5)
    rbf_blocks = bell_draw(splits[5], (FBLOCKS, BLOCK, SW), BLOCK ** -0.5, 0.5, ((0, 32),))
    block_owner_keys = jax.random.split(jax.random.fold_in(splits[6], 1), FBLOCKS // FB)
    block_owner_turns = jax.random.permutation(jax.random.fold_in(splits[6], 3), FBLOCKS // FB)
    block_owner = jax.vmap(lambda own, number: deal_out(jax.random.fold_in(splits[6], 2), own, number, FB, N_FLUID, 1, MOST, 2))(block_owner_keys, block_owner_turns).reshape((FBLOCKS, 1))
    block_row = touch_ends(jax.random.randint(splits[7], (FBLOCKS, 1), 0, SR), jax.random.fold_in(splits[7], 1), 0, SR - 1).astype(jnp.int32)
    displacement = bell_draw(splits[8], (NSR, 3, SW), 1.0, 6.0, ((0, 32),), jnp.float32)
    stiffness = jnp.clip(jnp.exp(math.log(4.0) - 2.0794415 * jax.random.uniform(splits[9], (NSR, SW), jnp.float32) ** level_of(splits[9], (NSR, SW), ((0, 32),), -0.2, 0.2)), 0.5, 4.0)
    residual_history = draw_residual_history(jax.random.fold_in(splits[12], 71), 0)
    solution_history = bell_draw(splits[11], (HIST, NSR, 3, SW), 1.0, 6.0, ((1, 32),), jnp.float32)
    return {"flow": flow, "wall_motion": wall_motion, "normal_operator": normal_operator, "wall_coupling": wall_coupling, "wall_stencil": wall_stencil, "rbf_blocks": rbf_blocks, "block_owner": block_owner, "block_row": block_row, "displacement": displacement, "stiffness": stiffness, "residual_history": residual_history, "solution_history": solution_history}


spread_rate = 0.25

def reference(flow, wall_motion, normal_operator, wall_coupling, wall_stencil, rbf_blocks, block_owner, block_row, displacement, stiffness, residual_history, solution_history):
    field = flow.astype(jnp.float32)
    drift = jnp.dot(flow.reshape(-1, NW).astype(jnp.float32), normal_operator.astype(jnp.float32), preferred_element_type=jnp.float32).reshape(field.shape)
    padded = jnp.pad(field, ((0, 0), (1, 1), (0, 0)))
    spread = padded[:, 2:, :] + padded[:, :-2, :] - 2.0 * field
    new_flow = (field + drift + spread_rate * spread + wall_motion[:, :, None] * wall_coupling[None, None, :]).astype(jnp.bfloat16)
    traction = jnp.dot(new_flow.reshape(-1, NW).astype(jnp.float32), wall_stencil.astype(jnp.float32), preferred_element_type=jnp.float32).astype(jnp.bfloat16)
    pieces = traction.reshape(3, FBLOCKS, BLOCK).astype(jnp.float32)
    rbf = rbf_blocks.astype(jnp.float32)
    mapped = jnp.einsum('cbp,bpq->bcq', pieces, rbf)
    home = (jnp.arange(FBLOCKS, dtype=jnp.int32) // FB % N_SOLID).astype(jnp.int32)
    target = ((block_owner[:, 0] * N_SOLID + home) * SR + block_row[:, 0]).astype(jnp.int32)
    force = jax.ops.segment_sum(mapped, target, NSR)
    solved = displacement
    denom = 4.0 + stiffness[:, None, :]
    for sweep in range(SWEEPS):
        rows = jnp.pad(solved, ((1, 1), (0, 0), (0, 0)))
        across = jnp.pad(solved, ((0, 0), (0, 0), (1, 1)))
        beside = rows[2:] + rows[:-2] + across[:, :, 2:] + across[:, :, :-2]
        solved = (force + beside) / denom
    residual = solved - displacement
    flat_res = residual_history.reshape(HIST, -1)
    flat = residual.reshape(-1)
    gram = jnp.dot(flat_res, flat_res.T, precision=lax.Precision.HIGHEST)
    proj = jnp.dot(flat_res, flat, precision=lax.Precision.HIGHEST)
    squares = jnp.sum(flat * flat)
    lower = jnp.linalg.cholesky(gram)
    coeff = jax.scipy.linalg.cho_solve((lower, True), -proj)
    update = jnp.dot(coeff, solution_history.reshape(HIST, -1), precision=lax.Precision.HIGHEST).reshape(solved.shape)
    next_displacement = solved + update
    shell = next_displacement.astype(jnp.bfloat16)
    picked = shell[target].astype(jnp.float32)
    wall_next = jnp.einsum('bpq,bcq->cbp', rbf, picked).reshape(3, NS)
    return (new_flow, next_displacement, wall_next, jnp.sqrt(squares))
```

```python
import jax
import jax.numpy as jnp
from jax import lax
from jax.experimental import pallas as pl
from jax.experimental.pallas import tpu as pltpu
from jax.sharding import PartitionSpec as P

SWEEPS = 4
AXES = ("fluid", "solid")
LANES = 128
spread_rate = 0.25
f32 = jnp.float32
bf16 = jnp.bfloat16
HIGHEST = lax.Precision.HIGHEST
VMEM = pltpu.MemorySpace.VMEM
SMEM = pltpu.MemorySpace.SMEM
ANY = pl.ANY


def up_to(value, step):
    return -(-value // step) * step


def dot(a, b, precision=None):
    return lax.dot_general(a, b, (((1,), (0,)), ((), ())), precision=precision, preferred_element_type=f32)


def dot_nt(a, b, precision=None):
    return lax.dot_general(a, b, (((1,), (1,)), ((), ())), precision=precision, preferred_element_type=f32)


def dot_tn(a, b, precision=None):
    return lax.dot_general(a, b, (((0,), (0,)), ((), ())), precision=precision, preferred_element_type=f32)


def iota(shape, dim):
    return lax.broadcasted_iota(jnp.int32, shape, dim)


def split3(value):
    high = value.astype(bf16)
    rest = value - high.astype(f32)
    middle = rest.astype(bf16)
    low = (rest - middle.astype(f32)).astype(bf16)
    return high, middle, low


def spec(memory):
    return pl.BlockSpec(memory_space=memory)


def largest_divisor(value, most):
    return max(d for d in range(1, most + 1) if value % d == 0)


def first_stage(me, owner, local_row, history, head, tail, devices, groups, inner, slots, capacity):
    count, lines, _ = history.shape
    comps = head.shape[0]
    blocks = owner.shape[1]
    part = count // groups
    half = part // 2
    chunk = largest_divisor(lines, 16)

    def kernel(me_ref, owner_ref, row_ref, hist_ref, head_ref, tail_ref, send_ref, chosen_ref, label_ref, turned, acc, sems):
        for k in range(lines):
            pltpu.make_async_copy(hist_ref.at[:, k, :], turned.at[k], sems.at[k]).start()
        send_ref[...] = jnp.zeros(send_ref.shape, f32)
        owners = owner_ref[...]
        names = jnp.where(owners == iota((groups, blocks), 0), 1.0, 0.0)
        before = jnp.where(iota((blocks, blocks), 0) < iota((blocks, blocks), 1), 1.0, 0.0)
        earlier = dot(names.astype(bf16), before.astype(bf16))
        numbers = (row_ref[...] + 1).astype(f32)
        place = iota((slots, blocks), 0).astype(f32)
        for g in range(groups):
            mine = jnp.where((earlier[g : g + 1] == place) & (names[g : g + 1] > 0.5), 1.0, 0.0)
            chosen_ref[g * slots : (g + 1) * slots, :] = mine.astype(bf16)
        labels = dot_nt(jnp.broadcast_to(numbers, (8, blocks)).astype(bf16), chosen_ref[...])
        for g in range(groups):
            label_ref[g : g + 1, :] = jnp.concatenate(
                [labels[0:1, g * slots : (g + 1) * slots], jnp.zeros((1, LANES - slots), f32)], axis=1
            )
        acc[...] = jnp.zeros(acc.shape, f32)

        def body(step, carry):
            pieces = []
            for k in range(chunk):
                line = step * chunk + k
                pltpu.make_async_copy(hist_ref.at[:, line, :], turned.at[line], sems.at[line]).wait()
                pieces.append(turned[line])
            parts = split3(jnp.concatenate(pieces, axis=1))
            left = jnp.concatenate(parts, axis=0)
            right = jnp.concatenate(parts + (jnp.zeros_like(parts[0]),), axis=0)
            acc[...] += dot_nt(left, right)
            return carry

        lax.fori_loop(0, lines // chunk, body, 0)
        total = acc[0:count, :] + acc[count : 2 * count, :] + acc[2 * count :, :]
        wide = total[:, :LANES] + total[:, LANES:]
        wide = wide + pltpu.roll(wide, LANES // 2, 1)
        low_lane = iota((half, LANES), 1) < LANES // 2
        for g in range(groups):
            packed = jnp.where(
                low_lane, wide[g * part : g * part + half], wide[g * part + half : (g + 1) * part]
            )
            for s in range(inner):
                send_ref[g * inner + s, 0:half, :] = packed
        own = me_ref[0]

        @pl.when(own > 0)
        def _():
            rows = head_ref[...].astype(f32)
            for c in range(comps):
                send_ref[own - 1, 4 + c : 5 + c, :] = rows[c, 0:1, :]

        @pl.when(own < devices - 1)
        def _():
            rows = tail_ref[...].astype(f32)
            for c in range(comps):
                send_ref[own + 1, 4 + c : 5 + c, :] = rows[c, 15:16, :]

    return pl.pallas_call(
        kernel,
        out_shape=(
            jax.ShapeDtypeStruct((devices, 8, LANES), f32),
            jax.ShapeDtypeStruct((groups * slots, blocks), bf16),
            jax.ShapeDtypeStruct((groups, LANES), f32),
        ),
        in_specs=[spec(SMEM), spec(VMEM), spec(VMEM), spec(ANY), spec(VMEM), spec(VMEM)],
        out_specs=(spec(VMEM), spec(VMEM), spec(VMEM)),
        scratch_shapes=[
            pltpu.VMEM((lines, count, LANES), f32),
            pltpu.VMEM((3 * count, 4 * count), f32),
            pltpu.SemaphoreType.DMA((lines,)),
        ],
        name="gram",
    )(me, owner, local_row, history, head, tail)


def flow_stage(flow, wall_motion, normal_operator, coupling, stencil, rbf, tile):
    comps, points, normal = flow.shape
    steps = points // tile
    inside = tile // LANES

    def kernel(flow_ref, prev_ref, next_ref, motion_ref, op_ref, coup_ref, sten_ref, rbf_ref, new_ref, map_ref, pre_ref, tr_ref, edge_ref, quarter, cols):
        i = pl.program_id(0)
        for c in range(comps):
            for j in range(inside):
                cols[c * inside + j : c * inside + j + 1, :] = motion_ref[c : c + 1, j * LANES : (j + 1) * LANES]
        turned = jnp.transpose(cols[...])
        coup = coup_ref[...]
        op = op_ref[...]
        sten = jnp.broadcast_to(sten_ref[...], (8, normal))
        row8 = iota((8, tile), 0)
        keep_prev = jnp.where(i > 0, spread_rate, 0.0)
        keep_next = jnp.where(i < steps - 1, spread_rate, 0.0)
        trac = None
        for c in range(comps):
            quarter[0:8, :] = prev_ref[c, 8:16, :].astype(f32) * keep_prev
            quarter[8 : 8 + tile, :] = flow_ref[c].astype(f32) * spread_rate
            quarter[8 + tile : 16 + tile, :] = next_ref[c, 0:8, :].astype(f32) * keep_next
            for j in range(inside):
                o = j * LANES
                drift = dot(flow_ref[c, o : o + LANES, :], op)
                mid = quarter[8 + o : 8 + o + LANES, :]
                around = quarter[7 + o : 7 + o + LANES, :] + quarter[9 + o : 9 + o + LANES, :]
                k = c * inside + j
                fresh = drift + (mid + mid) + around + turned[:, k : k + 1] * coup
                new_ref[c, o : o + LANES, :] = fresh.astype(bf16)
                if j == 0:

                    @pl.when(i == 0)
                    def _():
                        pre_ref[0, 4 + c : 5 + c, :] = fresh[0:1, :]
                        edge_ref[0, c] = fresh[0:16, :].astype(bf16)

                if j == inside - 1:

                    @pl.when(i == steps - 1)
                    def _():
                        pre_ref[1, 4 + c : 5 + c, :] = fresh[LANES - 1 : LANES, :]
                        edge_ref[1, c] = fresh[LANES - 16 : LANES, :].astype(bf16)

            row = dot_nt(sten, new_ref[c])
            trac = row if trac is None else jnp.where((row8 == c) | (row8 == 4 + c), row, trac)
        trac = trac.astype(bf16)

        @pl.when(i == 0)
        def _():
            tr_ref[0] = trac[:, 0:LANES].astype(f32)

        @pl.when(i == steps - 1)
        def _():
            tr_ref[1] = trac[:, tile - LANES : tile].astype(f32)

        for j in range(inside):
            got = dot(trac[:, j * LANES : (j + 1) * LANES], rbf_ref[j])
            for c in range(comps):
                map_ref[c, j : j + 1, :] = got[4 + c : 5 + c, :]

    per = tile // 16
    last = points // 16 - 1
    fixed2 = lambda i: (0, 0)
    return pl.pallas_call(
        kernel,
        grid=(steps,),
        out_shape=(
            jax.ShapeDtypeStruct(flow.shape, bf16),
            jax.ShapeDtypeStruct((comps, points // LANES, LANES), f32),
            jax.ShapeDtypeStruct((2, 8, LANES), f32),
            jax.ShapeDtypeStruct((2, 8, LANES), f32),
            jax.ShapeDtypeStruct((2, comps, 16, LANES), bf16),
        ),
        in_specs=[
            pl.BlockSpec((comps, tile, normal), lambda i: (0, i, 0)),
            pl.BlockSpec((comps, 16, normal), lambda i: (0, jnp.maximum(i * per - 1, 0), 0)),
            pl.BlockSpec((comps, 16, normal), lambda i: (0, jnp.minimum((i + 1) * per, last), 0)),
            pl.BlockSpec((comps, tile), lambda i: (0, i)),
            pl.BlockSpec((normal, normal), fixed2),
            pl.BlockSpec((1, normal), fixed2),
            pl.BlockSpec((1, normal), fixed2),
            pl.BlockSpec((inside, LANES, LANES), lambda i: (i, 0, 0)),
        ],
        out_specs=(
            pl.BlockSpec((comps, tile, normal), lambda i: (0, i, 0)),
            pl.BlockSpec((comps, inside, LANES), lambda i: (0, i, 0)),
            pl.BlockSpec((2, 8, LANES), lambda i: (0, 0, 0)),
            pl.BlockSpec((2, 8, LANES), lambda i: (0, 0, 0)),
            pl.BlockSpec((2, comps, 16, LANES), lambda i: (0, 0, 0, 0)),
        ),
        scratch_shapes=[pltpu.VMEM((tile + 16, LANES), f32), pltpu.VMEM((LANES, LANES), f32)],
        name="flow",
    )(flow, flow, flow, wall_motion, normal_operator, coupling, stencil, rbf)


def pack_stage(me, got, pre, tr, edge, stencil, rbf, mapped, chosen, labels, new_flow, devices, groups, slots, capacity, count, width):
    comps, blocks, _ = mapped.shape
    points = new_flow.shape[1]
    part = count // groups
    half = part // 2

    def kernel(me_ref, got_ref, pre_ref, tr_ref, edge_ref, sten_ref, rbf_first, rbf_last, map_ref, chosen_ref, label_ref, flow_in, flow_out, send_ref, tiles, sems):
        own = me_ref[0]
        sten = sten_ref[...].astype(f32)
        lane = iota((8, LANES), 1)
        row16 = iota((16, LANES), 0)
        fixed = []
        for e in range(2):
            if e == 0:
                halo = got_ref[jnp.maximum(own - 1, 0)] * jnp.where(own > 0, spread_rate, 0.0)
            else:
                halo = got_ref[jnp.minimum(own + 1, devices - 1)] * jnp.where(own < devices - 1, spread_rate, 0.0)
            fresh = (pre_ref[e] + halo).astype(bf16).astype(f32)
            at = 0 if e == 0 else 15
            for c in range(comps):
                tiles[e, c] = jnp.where(row16 == at, fresh[4 + c : 5 + c, :], edge_ref[e, c].astype(f32)).astype(bf16)
            start = 0 if e == 0 else points - 16
            pltpu.make_async_copy(tiles.at[e], flow_out.at[:, pl.ds(start, 16), :], sems.at[e]).start()
            point = jnp.sum(fresh * sten, axis=1, keepdims=True)
            trac = jnp.where(lane == (0 if e == 0 else LANES - 1), point, tr_ref[e]).astype(bf16)
            fixed.append(dot(trac, (rbf_first if e == 0 else rbf_last)[0]))
        total = got_ref[0]
        for d in range(1, devices):
            total = total + got_ref[d]
        swapped = pltpu.roll(pltpu.roll(total, LANES // 2, 1), half, 0)
        rows = iota((8, LANES), 0)
        gram = jnp.where(rows < half, total, swapped)
        gram = jnp.where(rows < part, gram, 0.0)
        pieces = split3(gram)
        block = iota((blocks, LANES), 0)
        label_row = iota((slots, LANES), 0) == capacity
        for c in range(comps):
            here = jnp.where(block == 0, fixed[0][4 + c : 5 + c, :], map_ref[c])
            here = jnp.where(block == blocks - 1, fixed[1][4 + c : 5 + c, :], here)
            out = dot(chosen_ref[...], here.astype(bf16))
            for g in range(groups):
                cut = out[g * slots : (g + 1) * slots, :]
                if c == 0:
                    cut = jnp.where(label_row, label_ref[g : g + 1, :], cut)
                send_ref[g, 0:slots, c * LANES : (c + 1) * LANES] = cut.astype(bf16)
                send_ref[g, slots : slots + 8, c * LANES : (c + 1) * LANES] = pieces[c]
        for e in range(2):
            start = 0 if e == 0 else points - 16
            pltpu.make_async_copy(tiles.at[e], flow_out.at[:, pl.ds(start, 16), :], sems.at[e]).wait()

    full = lambda a: pl.BlockSpec(a.shape, lambda i: (0,) * a.ndim)
    return pl.pallas_call(
        kernel,
        grid=(1,),
        out_shape=(
            jax.ShapeDtypeStruct(new_flow.shape, bf16),
            jax.ShapeDtypeStruct((groups, slots + 8, comps * width), bf16),
        ),
        in_specs=[
            spec(SMEM), full(got), full(pre), full(tr), full(edge), full(stencil),
            pl.BlockSpec((1, LANES, LANES), lambda i: (0, 0, 0)),
            pl.BlockSpec((1, LANES, LANES), lambda i: (blocks - 1, 0, 0)),
            full(mapped), full(chosen), full(labels), spec(ANY),
        ],
        out_specs=(spec(ANY), pl.BlockSpec((groups, slots + 8, comps * width), lambda i: (0, 0, 0))),
        scratch_shapes=[pltpu.VMEM((2, comps, 16, LANES), bf16), pltpu.SemaphoreType.DMA((2,))],
        input_output_aliases={11: 0},
        name="pack",
    )(me, got, pre, tr, edge, stencil, rbf, rbf, mapped, chosen, labels, new_flow)


def place_stage(arrived, displacement, stiffness, groups, slots, capacity, count):
    comps, rows, width = displacement.shape
    part = count // groups
    depth = SWEEPS
    short = depth - 1

    def kernel(got_ref, disp_ref, stiff_ref, force_ref, gram_ref, label_ref, head_ref, tail_ref):
        index = iota((rows, slots), 0).astype(f32) + 1.0
        total = jnp.zeros((rows, comps * width), f32)
        for g in range(groups):
            labels = got_ref[g, capacity : capacity + 1, 0:LANES].astype(f32)
            label_ref[g : g + 1, :] = labels
            placed = jnp.where(labels[:, 0:slots] == index, 1.0, 0.0).astype(bf16)
            total = total + dot(placed, got_ref[g, 0:slots, :])
            extra = got_ref[g, slots : slots + 8, :].astype(f32)
            value = extra[:, 0:LANES] + extra[:, LANES : 2 * LANES] + extra[:, 2 * LANES : 3 * LANES]
            gram_ref[g * part : (g + 1) * part, :] = value[0:part, 0:count]
        for c in range(comps):
            force_ref[c] = total[:, c * width : (c + 1) * width]
        for c in range(comps):
            head_ref[c * short : (c + 1) * short, :] = force_ref[c, 0:short, :]
            tail_ref[c * short : (c + 1) * short, :] = force_ref[c, rows - short : rows, :]
            at = comps * short + c * depth
            head_ref[at : at + depth, :] = disp_ref[c, 0:depth, :]
            tail_ref[at : at + depth, :] = disp_ref[c, rows - depth : rows, :]
        at = comps * (short + depth)
        head_ref[at : at + short, :] = stiff_ref[0:short, :]
        tail_ref[at : at + short, :] = stiff_ref[rows - short : rows, :]

    edge = (comps * (short + depth) + short, width)
    return pl.pallas_call(
        kernel,
        out_shape=(
            jax.ShapeDtypeStruct((comps, rows, width), f32),
            jax.ShapeDtypeStruct((count, count), f32),
            jax.ShapeDtypeStruct((groups, LANES), f32),
            jax.ShapeDtypeStruct(edge, f32),
            jax.ShapeDtypeStruct(edge, f32),
        ),
        name="place",
    )(arrived, displacement, stiffness)


def sweep_stage(me, force, displacement, stiffness, before, after, history, devices):
    comps, rows, width = displacement.shape
    count, lines, _ = history.shape
    depth = SWEEPS
    short = depth - 1
    rim = 8
    whole = rows + 2 * rim

    def kernel(me_ref, force_ref, disp_ref, stiff_ref, before_ref, after_ref, hist_ref, solved_ref, send_ref, ext, sums):
        own = me_ref[0]
        row = iota((whole, width), 0)
        lane = iota((whole, width), 1)
        lowest = jnp.where(own > 0, rim - depth, rim)
        highest = jnp.where(own < devices - 1, rim + rows + depth, rim + rows)
        valid = jnp.where((row >= lowest) & (row < highest), 1.0, 0.0)
        at = comps * (short + depth)
        ext[...] = jnp.zeros(ext.shape, f32)
        ext[0, rim - short : rim, :] = before_ref[at : at + short, :]
        ext[0, rim : rim + rows, :] = stiff_ref[...]
        ext[0, rim + rows : rim + rows + short, :] = after_ref[at : at + short, :]
        scale = valid / (4.0 + ext[0])
        left_ok = jnp.where(lane > 0, 1.0, 0.0)
        right_ok = jnp.where(lane < width - 1, 1.0, 0.0)
        squares = jnp.zeros((8, width), f32)
        residuals = []
        for c in range(comps):
            f = 1 + 2 * c
            ext[f, rim - short : rim, :] = before_ref[c * short : (c + 1) * short, :]
            ext[f, rim : rim + rows, :] = force_ref[c]
            ext[f, rim + rows : rim + rows + short, :] = after_ref[c * short : (c + 1) * short, :]
            d = comps * short + c * depth
            ext[f + 1, rim - depth : rim, :] = before_ref[d : d + depth, :]
            ext[f + 1, rim : rim + rows, :] = disp_ref[c]
            ext[f + 1, rim + rows : rim + rows + depth, :] = after_ref[d : d + depth, :]
        for c in range(comps):
            push = ext[1 + 2 * c]
            solved = ext[2 + 2 * c]
            for sweep in range(SWEEPS):
                beside = pltpu.roll(solved, 1, 0) + pltpu.roll(solved, whole - 1, 0)
                beside = beside + pltpu.roll(solved, 1, 1) * left_ok + pltpu.roll(solved, width - 1, 1) * right_ok
                solved = (push + beside) * scale
            mine = solved[rim : rim + rows, :]
            solved_ref[c] = mine
            residual = mine - disp_ref[c]
            residuals.append(residual)
            square = residual * residual
            for k in range(rows // 8):
                squares = squares + square[8 * k : 8 * k + 8, :]
        sums[count:, :] = jnp.zeros((LANES - count, width), f32)
        sums[count : count + 1, :] = jnp.sum(squares, axis=0, keepdims=True)
        flat = jnp.concatenate(residuals, axis=0)
        for j in range(count):
            prod = hist_ref[j] * flat
            sums[j : j + 1, :] = jnp.sum(prod, axis=0, keepdims=True)
        line = dot_nt(jnp.ones((8, width), f32), sums[...], HIGHEST)
        for d in range(devices):
            send_ref[d] = line[0:1, :]

    return pl.pallas_call(
        kernel,
        out_shape=(
            jax.ShapeDtypeStruct((comps, rows, width), f32),
            jax.ShapeDtypeStruct((devices, 1, LANES), f32),
        ),
        in_specs=[spec(SMEM)] + [spec(VMEM)] * 6,
        out_specs=(spec(VMEM), spec(VMEM)),
        scratch_shapes=[pltpu.VMEM((1 + 2 * comps, whole, width), f32), pltpu.VMEM((LANES, width), f32)],
        name="sweeps",
    )(me, force, displacement, stiffness, before, after, history)


def update_stage(arrived, inverse, inverse_t, history, solved, labels, groups, slots):
    comps, rows, width = solved.shape
    count, lines, _ = history.shape

    def kernel(got_ref, inv_ref, invt_ref, hist_ref, solved_ref, label_ref, next_ref, reply_ref, line_ref, coeff):
        line = jnp.sum(got_ref[...], axis=0)
        line_ref[...] = line
        half = jnp.sum(inv_ref[...] * line[:, 0:count], axis=1, keepdims=True)
        coeff[...] = -dot(invt_ref[...], jnp.broadcast_to(half, (count, width)), HIGHEST)

        def body(j, total):
            return total + hist_ref[j] * coeff[pl.ds(j, 1), :]

        update = lax.fori_loop(0, count, body, jnp.zeros((lines, width), f32), unroll=8)
        shell = []
        for c in range(comps):
            fresh = solved_ref[c] + update[c * rows : (c + 1) * rows, :]
            next_ref[c] = fresh
            shell.append(fresh.astype(bf16))
        shell = jnp.concatenate(shell, axis=1)
        index = iota((rows, slots), 0).astype(f32) + 1.0
        for g in range(groups):
            placed = jnp.where(label_ref[g : g + 1, 0:slots] == index, 1.0, 0.0).astype(bf16)
            reply_ref[g] = dot_tn(placed, shell).astype(bf16)

    return pl.pallas_call(
        kernel,
        out_shape=(
            jax.ShapeDtypeStruct((comps, rows, width), f32),
            jax.ShapeDtypeStruct((groups, slots, comps * width), bf16),
            jax.ShapeDtypeStruct((1, LANES), f32),
        ),
        scratch_shapes=[pltpu.VMEM((count, width), f32)],
        name="update",
    )(arrived, inverse, inverse_t, history, solved, labels)


def wall_stage(returned, chosen, rbf, comps):
    blocks, block, width = rbf.shape
    groups, slots, _ = returned.shape

    def kernel(got_ref, chosen_ref, rbf_ref, out_ref, shells):
        got = jnp.concatenate([got_ref[g] for g in range(groups)], axis=0)
        fetched = dot_tn(chosen_ref[...], got)
        shells[...] = jnp.zeros(shells.shape, f32)
        for c in range(comps):
            shells[:, c, :] = fetched[:, c * width : (c + 1) * width]
        for b in range(blocks):
            res = dot_nt(shells[b].astype(bf16), rbf_ref[b])
            out_ref[:, b * block : (b + 1) * block] = res[0:comps, :]

    return pl.pallas_call(
        kernel,
        out_shape=jax.ShapeDtypeStruct((comps, blocks * block), f32),
        scratch_shapes=[pltpu.VMEM((blocks, 8, width), f32)],
        name="wall",
    )(returned, chosen, rbf)


def per_device(
    flow,
    wall_motion,
    normal_operator,
    wall_coupling,
    wall_stencil,
    rbf_blocks,
    block_owner,
    block_row,
    displacement,
    stiffness,
    residual_history,
    solution_history,
):
    groups = lax.axis_size("fluid")
    inner = lax.axis_size("solid")
    devices = groups * inner
    comps, points, normal = flow.shape
    blocks, block, width = rbf_blocks.shape
    count = residual_history.shape[0]
    rows = displacement.shape[0]
    capacity = max(2, (3 * blocks + 2 * groups - 1) // (2 * groups))
    slots = up_to(capacity + 1, 16)
    me = lax.axis_index(AXES).astype(jnp.int32).reshape(1)

    disp = displacement.transpose(1, 0, 2)
    res_hist = residual_history.transpose(0, 2, 1, 3).reshape(count, comps * rows, width)
    sol_hist = solution_history.transpose(0, 2, 1, 3).reshape(count, comps * rows, width)
    owner = block_owner.reshape(1, blocks)
    local_row = block_row.reshape(1, blocks)
    coupling = wall_coupling.reshape(1, normal)
    stencil = wall_stencil.reshape(1, normal)

    send, chosen, labels = first_stage(
        me, owner, local_row, res_hist, flow[:, :16, :], flow[:, points - 16 :, :], devices, groups, inner, slots, capacity
    )
    got = lax.all_to_all(send, AXES, 0, 0, tiled=True)
    tile = 1024 if points % 1024 == 0 else points
    new_flow, mapped, pre, tr, edge = flow_stage(
        flow, wall_motion, normal_operator, coupling, stencil, rbf_blocks, tile
    )
    new_flow, send = pack_stage(
        me, got, pre, tr, edge, stencil, rbf_blocks, mapped, chosen, labels, new_flow,
        devices, groups, slots, capacity, count, width,
    )
    arrived = lax.all_to_all(send, "fluid", 0, 0, tiled=True)
    force, gram, placed_labels, head, tail = place_stage(arrived, disp, stiffness, groups, slots, capacity, count)
    before = lax.ppermute(tail, AXES, [(i, i + 1) for i in range(devices - 1)])
    after = lax.ppermute(head, AXES, [(i + 1, i) for i in range(devices - 1)])
    lower = jnp.linalg.cholesky(gram)
    inverse = jax.scipy.linalg.solve_triangular(lower, jnp.eye(count, dtype=f32), lower=True)
    solved, send = sweep_stage(me, force, disp, stiffness, before, after, res_hist, devices)
    got = lax.all_to_all(send, AXES, 0, 0, tiled=True)
    fresh, reply, line = update_stage(got, inverse, inverse.T, sol_hist, solved, placed_labels, groups, slots)
    returned = lax.all_to_all(reply, "fluid", 0, 0, tiled=True)
    wall_next = wall_stage(returned, chosen, rbf_blocks, comps)
    return (new_flow, fresh.transpose(1, 0, 2), wall_next, jnp.sqrt(line[0, count]))


def solution(mesh):
    return jax.shard_map(
        per_device,
        mesh=mesh,
        in_specs=(
            P(None, ("fluid", "solid"), None),
            P(None, ("fluid", "solid")),
            P(),
            P(),
            P(),
            P(("fluid", "solid"), None, None),
            P(("fluid", "solid"), None),
            P(("fluid", "solid"), None),
            P(("fluid", "solid"), None, None),
            P(("fluid", "solid"), None),
            P(None, ("fluid", "solid"), None, None),
            P(None, ("fluid", "solid"), None, None),
        ),
        out_specs=(
            P(None, ("fluid", "solid"), None),
            P(("fluid", "solid"), None, None),
            P(None, ("fluid", "solid")),
            P(),
        ),
        check_vma=False,
    )
```

```python
import jax
import jax.numpy as jnp
from jax import lax
from jax.experimental import pallas as pl
from jax.experimental.pallas import tpu as pltpu
from jax.sharding import PartitionSpec as P

SWEEPS = 4
AXES = ("fluid", "solid")
LANES = 128
spread_rate = 0.25
f32 = jnp.float32
bf16 = jnp.bfloat16
HIGHEST = lax.Precision.HIGHEST
VMEM = pltpu.MemorySpace.VMEM
SMEM = pltpu.MemorySpace.SMEM
ANY = pl.ANY
PARAMS = pltpu.CompilerParams(vmem_limit_bytes=24 * 2**20)


def up_to(value, step):
    return -(-value // step) * step


def dot(a, b, precision=None):
    return lax.dot_general(a, b, (((1,), (0,)), ((), ())), precision=precision, preferred_element_type=f32)


def dot_nt(a, b, precision=None):
    return lax.dot_general(a, b, (((1,), (1,)), ((), ())), precision=precision, preferred_element_type=f32)


def dot_tn(a, b, precision=None):
    return lax.dot_general(a, b, (((0,), (0,)), ((), ())), precision=precision, preferred_element_type=f32)


def iota(shape, dim):
    return lax.broadcasted_iota(jnp.int32, shape, dim)


def split3(value):
    high = value.astype(bf16)
    rest = value - high.astype(f32)
    middle = rest.astype(bf16)
    low = (rest - middle.astype(f32)).astype(bf16)
    return high, middle, low


def spec(memory):
    return pl.BlockSpec(memory_space=memory)


def largest_divisor(value, most):
    return max(d for d in range(1, most + 1) if value % d == 0)


def in_vmem(value):
    return pltpu.with_memory_space_constraint(value, VMEM)


def in_hbm(value):
    return pltpu.with_memory_space_constraint(value, pltpu.MemorySpace.HBM)


def gram_stage(owner, local_row, history, groups, slots):
    count, lines, _ = history.shape
    blocks = owner.shape[1]
    part = count // groups
    chunk = largest_divisor(lines, 16)
    pitch = lines + 8

    def kernel(owner_hbm, row_hbm, hist_ref, gram_ref, chosen_ref, label_ref, held_ref, owner_ref, row_ref, sems):
        small = [
            pltpu.make_async_copy(owner_hbm, owner_ref, sems.at[lines // chunk]),
            pltpu.make_async_copy(row_hbm, row_ref, sems.at[lines // chunk + 1]),
        ]
        for copy in small:
            copy.start()
        copies = [
            pltpu.make_async_copy(
                hist_ref.at[:, pl.ds(k * chunk, chunk), :], held_ref.at[:, pl.ds(k * chunk, chunk), :], sems.at[k]
            )
            for k in range(lines // chunk)
        ]
        for copy in copies:
            copy.start()
        for copy in small:
            copy.wait()
        owners = owner_ref[...]
        names = jnp.where(owners == iota((groups, blocks), 0), 1.0, 0.0)
        before = jnp.where(iota((blocks, blocks), 0) < iota((blocks, blocks), 1), 1.0, 0.0)
        earlier = dot(names.astype(bf16), before.astype(bf16))
        numbers = (row_ref[...] + 1).astype(f32)
        place = iota((slots, blocks), 0).astype(f32)
        for g in range(groups):
            mine = jnp.where((earlier[g : g + 1] == place) & (names[g : g + 1] > 0.5), 1.0, 0.0)
            chosen_ref[g * slots : (g + 1) * slots, :] = mine.astype(bf16)
        labels = dot_nt(jnp.broadcast_to(numbers, (8, blocks)).astype(bf16), chosen_ref[...])
        for g in range(groups):
            label_ref[g : g + 1, :] = jnp.concatenate(
                [labels[0:1, g * slots : (g + 1) * slots], jnp.zeros((1, LANES - slots), f32)], axis=1
            )
        flat = held_ref.reshape(count * pitch, LANES)
        acc = None
        for k in range(lines // chunk):
            copies[k].wait()
            cut = [flat[pl.ds(k * chunk + i, count, stride=pitch), :] for i in range(chunk)]
            parts = split3(jnp.concatenate(cut, axis=1))
            left = jnp.concatenate(parts, axis=0)
            right = jnp.concatenate(parts + (jnp.zeros_like(parts[0]),), axis=0)
            prod = dot_nt(left, right)
            acc = prod if acc is None else acc + prod
        total = acc[0:count, :] + acc[count : 2 * count, :] + acc[2 * count :, :]
        wide = total[:, :LANES] + total[:, LANES:]
        wide = wide + pltpu.roll(wide, LANES // 2, 1)
        pieces = split3(wide)
        for g in range(groups):
            for k in range(3):
                cut = pieces[k][g * part : (g + 1) * part, :]
                if part < 8:
                    cut = jnp.concatenate([cut.astype(f32), jnp.zeros((8 - part, LANES), f32)], axis=0).astype(bf16)
                gram_ref[g, :, k * LANES : (k + 1) * LANES] = cut

    return pl.pallas_call(
        kernel,
        out_shape=(
            VMEM((groups, 8, 3 * LANES), bf16),
            VMEM((groups * slots, blocks), bf16),
            VMEM((groups, LANES), f32),
        ),
        in_specs=[spec(ANY), spec(ANY), spec(ANY)],
        out_specs=(spec(VMEM), spec(VMEM), spec(VMEM)),
        scratch_shapes=[
            pltpu.VMEM((count, pitch, LANES), f32),
            pltpu.VMEM(owner.shape, jnp.int32),
            pltpu.VMEM(owner.shape, jnp.int32),
            pltpu.SemaphoreType.DMA((lines // chunk + 2,)),
        ],
        name="gram",
        compiler_params=PARAMS,
    )(in_hbm(owner), in_hbm(local_row), in_hbm(history))


def flow_stage(flow, head, tail, wall_motion, normal_operator, coupling, stencil, rbf, chosen, labels, gram, tile, slots, capacity):
    comps, points, normal = flow.shape
    groups = gram.shape[0]
    blocks = rbf.shape[0]
    steps = points // tile
    inside = tile // LANES
    names = comps * inside

    def kernel(flow_hbm, head_ref, tail_ref, motion_hbm, op_hbm, coup_hbm, sten_hbm, rbf_hbm, chosen_ref, label_ref, gram_ref, new_hbm, send_ref, held, fresh_ref, motion_ref, op_ref, coup_ref, sten_ref, rbf_ref, cols, turns, maps, quarter, outer, points_ref, sems, into, out):
        small = [
            pltpu.make_async_copy(coup_hbm, coup_ref, sems.at[0]),
            pltpu.make_async_copy(motion_hbm, motion_ref, sems.at[1]),
            pltpu.make_async_copy(op_hbm, op_ref, sems.at[2]),
            pltpu.make_async_copy(sten_hbm, sten_ref, sems.at[3]),
        ]
        rbf_copy = pltpu.make_async_copy(rbf_hbm, rbf_ref, sems.at[4])

        def load(t):
            at = pl.ds(pl.multiple_of(t * tile, tile), tile)
            return pltpu.make_async_copy(flow_hbm.at[:, at, :], held.at[:, at, :], into.at[t])

        def store(t):
            at = pl.ds(pl.multiple_of(t * tile, tile), tile)
            return pltpu.make_async_copy(fresh_ref.at[:, at, :], new_hbm.at[:, at, :], out.at[t])

        for copy in small:
            copy.start()
        load(0).start()
        load(1).start()
        rbf_copy.start()
        for t in range(2, steps):
            load(t).start()
        small[0].wait()
        high, middle, _ = split3(coup_ref[...])
        rows = iota((LANES, LANES), 0)
        value = jnp.where(rows < 2 * names, high.astype(f32), 0.0)
        value = jnp.where((rows >= 2 * names) & (rows < 3 * names), middle.astype(f32), value)
        value = jnp.where((rows >= 3 * names) & (rows < 4 * names), high.astype(f32), value)
        value = jnp.where((rows >= 4 * names) & (rows < 5 * names), middle.astype(f32), value)
        for copy in small[1:]:
            copy.wait()
        outer[0:normal, :] = op_ref[...]
        outer[normal:, :] = value.astype(bf16)
        which = lax.rem(iota((1, LANES), 1), names)
        sten = sten_ref[...].astype(f32)
        eye = iota((LANES, LANES), 0) == iota((LANES, LANES), 1)
        points_ref[...] = jnp.zeros(points_ref.shape, f32)
        for t in range(steps):
            for c in range(comps):
                for j in range(inside):
                    o = t * tile + j * LANES
                    cols[t, c * inside + j : c * inside + j + 1, :] = motion_ref[c : c + 1, o : o + LANES]
            high, middle, low = [piece.astype(f32) for piece in split3(cols[t, 0:names, :])]
            parts = [high, middle, high, low, middle, jnp.zeros((LANES - 5 * names, LANES), f32)]
            turns[t] = jnp.transpose(jnp.concatenate(parts, axis=0)).astype(bf16)
        load(0).wait()
        rbf_copy.wait()

        def mapping(first):
            for j in range(inside):
                got = dot(points_ref[first + j].astype(bf16), rbf_ref[first + j])
                for c in range(comps):
                    maps[c, pl.ds(first + j, 1), :] = got[c : c + 1, :]

        def step(i, carry, ahead=True):
            base = pl.multiple_of(i * tile, tile)
            if ahead:
                load(i + 1).wait()
            mapping(jnp.maximum(i - 1, 0) * inside)
            turned = turns[i]
            before = pl.multiple_of(jnp.maximum(base - 16, 0), 16)
            after = pl.multiple_of(jnp.minimum(base + tile, points - 16), 16)
            for c in range(comps):
                above = jnp.where(i > 0, held[c, pl.ds(before, 16), :].astype(f32)[15:16, :], tail_ref[c].astype(f32))
                below = jnp.where(i < steps - 1, held[c, pl.ds(after, 16), :].astype(f32)[0:1, :], head_ref[c].astype(f32))
                quarter[c, 7:8, :] = above * spread_rate
                quarter[c, 8 + tile : 9 + tile, :] = below * spread_rate
                quarter[c, 8 : 8 + tile, :] = held[c, pl.ds(base, tile), :].astype(f32) * spread_rate
                motion = [turned * jnp.where(which == c * inside + j, 1.0, 0.0).astype(bf16) for j in range(inside)]
                moved = dot(jnp.concatenate([held[c, pl.ds(base, tile), :], jnp.concatenate(motion, axis=0)], axis=1), outer[...])
                for j in range(inside):
                    o = j * LANES
                    at = pl.ds(pl.multiple_of(base + o, LANES), LANES)
                    fresh = moved[o : o + LANES, :]
                    mid = quarter[c, 8 + o : 8 + o + LANES, :]
                    around = quarter[c, 7 + o : 7 + o + LANES, :] + quarter[c, 9 + o : 9 + o + LANES, :]
                    fresh = (fresh + ((mid + mid) + around)).astype(bf16)
                    fresh_ref[c, at, :] = fresh
                    point = jnp.sum(fresh.astype(f32) * sten, axis=1, keepdims=True)
                    points_ref[i * inside + j, c : c + 1, :] = jnp.sum(jnp.where(eye, point, 0.0), axis=0, keepdims=True)
            store(i).start()
            return carry

        lax.fori_loop(0, steps - 1, step, 0)
        step(steps - 1, 0, ahead=False)
        mapping((steps - 1) * inside)
        label_row = iota((slots, LANES), 0) == capacity
        for g in range(groups):
            send_ref[g, slots : slots + 8, :] = gram_ref[g]
        for c in range(comps):
            out_c = dot(chosen_ref[...], maps[c].astype(bf16))
            for g in range(groups):
                cut = out_c[g * slots : (g + 1) * slots, :]
                if c == 0:
                    cut = jnp.where(label_row, label_ref[g : g + 1, :], cut)
                send_ref[g, 0:slots, c * LANES : (c + 1) * LANES] = cut.astype(bf16)
        for t in range(steps):
            store(t).wait()

    return pl.pallas_call(
        kernel,
        out_shape=(
            jax.ShapeDtypeStruct(flow.shape, bf16),
            VMEM((groups, slots + 8, comps * LANES), bf16),
        ),
        in_specs=[spec(ANY), spec(VMEM), spec(VMEM)] + [spec(ANY)] * 5 + [spec(VMEM)] * 3,
        out_specs=(spec(ANY), spec(VMEM)),
        scratch_shapes=[
            pltpu.VMEM(flow.shape, bf16),
            pltpu.VMEM(flow.shape, bf16),
            pltpu.VMEM(wall_motion.shape, f32),
            pltpu.VMEM(normal_operator.shape, bf16),
            pltpu.VMEM(coupling.shape, f32),
            pltpu.VMEM(stencil.shape, bf16),
            pltpu.VMEM(rbf.shape, bf16),
            pltpu.VMEM((steps, names, LANES), f32),
            pltpu.VMEM((steps, LANES, LANES), bf16),
            pltpu.VMEM((comps, blocks, LANES), f32),
            pltpu.VMEM((comps, tile + 16, LANES), f32),
            pltpu.VMEM((2 * LANES, LANES), bf16),
            pltpu.VMEM((blocks, 8, LANES), f32),
            pltpu.SemaphoreType.DMA((5,)),
            pltpu.SemaphoreType.DMA((steps,)),
            pltpu.SemaphoreType.DMA((steps,)),
        ],
        name="flow",
        compiler_params=PARAMS,
    )(in_hbm(flow), in_vmem(head), in_vmem(tail), in_hbm(wall_motion), in_hbm(normal_operator), in_hbm(coupling), in_hbm(stencil), in_hbm(rbf), in_vmem(chosen), in_vmem(labels), in_vmem(gram))


def place_stage(arrived, displacement, stiffness, slots, capacity, count):
    comps, rows, width = displacement.shape
    groups = arrived.shape[0]
    part = count // groups
    half = part // 2
    depth = SWEEPS
    short = depth - 1

    def kernel(got_ref, disp_ref, stiff_ref, force_ref, gram_ref, label_ref, head_ref, tail_ref):
        index = iota((rows, slots), 0).astype(f32) + 1.0
        total = jnp.zeros((rows, comps * width), f32)
        extra = jnp.zeros((8, 3 * LANES), f32)
        for g in range(groups):
            labels = got_ref[g, capacity : capacity + 1, 0:LANES].astype(f32)
            label_ref[g : g + 1, :] = labels
            placed = jnp.where(labels[:, 0:slots] == index, 1.0, 0.0).astype(bf16)
            total = total + dot(placed, got_ref[g, 0:slots, :])
            extra = extra + got_ref[g, slots : slots + 8, :].astype(f32)
        for c in range(comps):
            force_ref[c] = total[:, c * width : (c + 1) * width]
        gram = extra[:, 0:LANES] + extra[:, LANES : 2 * LANES] + extra[:, 2 * LANES : 3 * LANES]
        lower = pltpu.roll(gram, 8 - half, 0)
        gram_ref[...] = jnp.where(iota((8, LANES), 1) < LANES // 2, gram, lower)
        for c in range(comps):
            head_ref[c * short : (c + 1) * short, :] = total[0:short, c * width : (c + 1) * width]
            tail_ref[c * short : (c + 1) * short, :] = total[rows - short : rows, c * width : (c + 1) * width]
            at = comps * short + c * depth
            head_ref[at : at + depth, :] = disp_ref[c, 0:depth, :]
            tail_ref[at : at + depth, :] = disp_ref[c, rows - depth : rows, :]
        at = comps * (short + depth)
        head_ref[at : at + short, :] = stiff_ref[0:short, :]
        tail_ref[at : at + short, :] = stiff_ref[rows - short : rows, :]

    edge = (comps * (short + depth) + short, width)
    return pl.pallas_call(
        kernel,
        out_shape=(
            VMEM((comps, rows, width), f32),
            VMEM((8, LANES), f32),
            VMEM((groups, LANES), f32),
            VMEM(edge, f32),
            VMEM(edge, f32),
        ),
        name="place",
        compiler_params=PARAMS,
    )(in_vmem(arrived), in_vmem(displacement), in_vmem(stiffness))


def sweep_stage(me, force, displacement, stiffness, before, after, held, gram, half, devices):
    comps, rows, width = displacement.shape
    count = held.shape[0]
    depth = SWEEPS
    short = depth - 1
    rim = 8
    whole = rows + 2 * rim

    def kernel(me_ref, force_ref, disp_ref, stiff_ref, before_ref, after_ref, hist_ref, gram_ref, solved_ref, send_ref, ext, sums):
        own = me_ref[0]
        row = iota((whole, width), 0)
        lane = iota((whole, width), 1)
        lowest = jnp.where(own > 0, rim - depth, rim)
        highest = jnp.where(own < devices - 1, rim + rows + depth, rim + rows)
        valid = jnp.where((row >= lowest) & (row < highest), 1.0, 0.0)
        at = comps * (short + depth)
        ext[...] = jnp.zeros(ext.shape, f32)
        ext[0, rim - short : rim, :] = before_ref[at : at + short, :]
        ext[0, rim : rim + rows, :] = stiff_ref[...]
        ext[0, rim + rows : rim + rows + short, :] = after_ref[at : at + short, :]
        scale = valid / (4.0 + ext[0])
        left_ok = jnp.where(lane > 0, 1.0, 0.0)
        right_ok = jnp.where(lane < width - 1, 1.0, 0.0)
        squares = jnp.zeros((8, width), f32)
        residuals = []
        for c in range(comps):
            f = 1 + 2 * c
            ext[f, rim - short : rim, :] = before_ref[c * short : (c + 1) * short, :]
            ext[f, rim : rim + rows, :] = force_ref[c]
            ext[f, rim + rows : rim + rows + short, :] = after_ref[c * short : (c + 1) * short, :]
            d = comps * short + c * depth
            ext[f + 1, rim - depth : rim, :] = before_ref[d : d + depth, :]
            ext[f + 1, rim : rim + rows, :] = disp_ref[c]
            ext[f + 1, rim + rows : rim + rows + depth, :] = after_ref[d : d + depth, :]
        push = [ext[1 + 2 * c] for c in range(comps)]
        solved = [ext[2 + 2 * c] for c in range(comps)]
        for sweep in range(SWEEPS):
            for c in range(comps):
                old = solved[c]
                beside = pltpu.roll(old, 1, 0) + pltpu.roll(old, whole - 1, 0)
                beside = beside + pltpu.roll(old, 1, 1) * left_ok + pltpu.roll(old, width - 1, 1) * right_ok
                solved[c] = (push[c] + beside) * scale
        for c in range(comps):
            mine = solved[c][rim : rim + rows, :]
            solved_ref[c] = mine
            residual = mine - disp_ref[c]
            residuals.append(residual)
            square = residual * residual
            for k in range(rows // 8):
                squares = squares + square[8 * k : 8 * k + 8, :]
        sums[count:, :] = jnp.zeros((LANES - count, width), f32)
        sums[count : count + 1, :] = jnp.sum(squares, axis=0, keepdims=True)
        flat = jnp.concatenate(residuals, axis=0)
        for j in range(count):
            prod = hist_ref[j, 0 : comps * rows, :] * flat
            sums[j : j + 1, :] = jnp.sum(prod, axis=0, keepdims=True)
        line = dot_nt(jnp.ones((8, width), f32), sums[...], HIGHEST)
        chunk = jnp.where(iota((8, LANES), 0) < half, gram_ref[...], line)
        for d in range(devices):
            send_ref[d] = chunk

    return pl.pallas_call(
        kernel,
        out_shape=(
            VMEM((comps, rows, width), f32),
            VMEM((devices, 8, LANES), f32),
        ),
        in_specs=[spec(SMEM)] + [spec(VMEM)] * 7,
        out_specs=(spec(VMEM), spec(VMEM)),
        scratch_shapes=[pltpu.VMEM((1 + 2 * comps, whole, width), f32), pltpu.VMEM((LANES, width), f32)],
        name="sweeps",
        compiler_params=PARAMS,
    )(me, in_vmem(force), in_vmem(displacement), in_vmem(stiffness), in_vmem(before), in_vmem(after), in_vmem(held), in_vmem(gram))


def eliminate(rows):
    sub = iota((8, LANES), 0)
    number = len(rows)
    for p in range(number):
        cols = [[jnp.broadcast_to(rows[v][:, 8 * p + i : 8 * p + i + 1], (8, LANES)) for i in range(8)] for v in range(number)]
        pivot = rows[p]
        diag = list(cols[p])
        for i in range(8):
            inverse = 1.0 / diag[i][i : i + 1, :]
            factor = jnp.where(sub == i, 0.0, diag[i])
            line = pivot[i : i + 1, :] * inverse
            pivot = jnp.where(sub == i, line, pivot) - factor * line
            for j in range(i + 1, 8):
                edge = diag[j][i : i + 1, :] * inverse
                diag[j] = jnp.where(sub == i, edge, diag[j]) - factor * edge
        for v in range(number):
            if v != p:
                value = rows[v]
                for i in range(8):
                    value = value - cols[v][i] * pivot[i : i + 1, :]
                rows[v] = value
        rows[p] = pivot
    return rows


def update_stage(arrived, history, solved, labels, count, slots):
    comps, rows, width = solved.shape
    lines = history.shape[1]
    groups = labels.shape[0]
    devices = arrived.shape[0]
    inner = devices // groups
    part = count // groups
    half = part // 2

    def kernel(got_ref, hist_hbm, solved_ref, label_ref, next_ref, reply_ref, line_ref, table, coeff, hist_ref, sem):
        fetch = pltpu.make_async_copy(hist_hbm, hist_ref, sem)
        fetch.start()
        line = got_ref[0]
        for d in range(1, devices):
            line = line + got_ref[d]
        line = line[half : half + 1, :]
        line_ref[...] = line
        for g in range(groups):
            packed = got_ref[g * inner]
            for s in range(1, inner):
                packed = packed + got_ref[g * inner + s]
            table[g * part : g * part + half, :] = packed[0:half, :]
            table[g * part + half : (g + 1) * part, :] = pltpu.roll(packed, LANES // 2, 1)[0:half, :]
        lane = iota((8, LANES), 1)
        sub = iota((8, LANES), 0)
        system = []
        for v in range(count // 8):
            own = jnp.sum(jnp.where(lane == sub + 8 * v, line, 0.0), axis=1, keepdims=True)
            value = jnp.where(lane < count, table[8 * v : 8 * v + 8, :], 0.0)
            system.append(jnp.where(lane == count, -own, value))
        system = eliminate(system)
        for v in range(count // 8):
            coeff[8 * v : 8 * v + 8, :] = jnp.broadcast_to(system[v][:, count : count + 1], (8, LANES))

        fetch.wait()

        def body(j, total):
            return total + hist_ref[j] * coeff[pl.ds(j, 1), :]

        update = lax.fori_loop(0, count, body, jnp.zeros((lines, width), f32), unroll=8)
        shell = []
        for c in range(comps):
            fresh = solved_ref[c] + update[c * rows : (c + 1) * rows, :]
            next_ref[c] = fresh
            shell.append(fresh.astype(bf16))
        shell = jnp.concatenate(shell, axis=1)
        index = iota((rows, slots), 0).astype(f32) + 1.0
        for g in range(groups):
            placed = jnp.where(label_ref[g : g + 1, 0:slots] == index, 1.0, 0.0).astype(bf16)
            reply_ref[g] = dot_tn(placed, shell).astype(bf16)

    return pl.pallas_call(
        kernel,
        out_shape=(
            VMEM((comps, rows, width), f32),
            VMEM((groups, slots, comps * width), bf16),
            VMEM((1, LANES), f32),
        ),
        in_specs=[spec(VMEM), spec(ANY), spec(VMEM), spec(VMEM)],
        scratch_shapes=[
            pltpu.VMEM((count, LANES), f32),
            pltpu.VMEM((count, width), f32),
            pltpu.VMEM((count, lines, width), f32),
            pltpu.SemaphoreType.DMA,
        ],
        name="update",
        compiler_params=PARAMS,
    )(in_vmem(arrived), in_hbm(history), in_vmem(solved), in_vmem(labels))


def wall_stage(returned, chosen, rbf, comps):
    blocks, block, width = rbf.shape
    groups, slots, _ = returned.shape

    pieces = largest_divisor(blocks, 4)
    each = blocks // pieces

    def kernel(got_ref, chosen_ref, rbf_hbm, out_hbm, shells, rbf_ref, out_ref, sems, outs):
        copies = [
            pltpu.make_async_copy(rbf_hbm.at[pl.ds(k * each, each)], rbf_ref.at[pl.ds(k * each, each)], sems.at[k])
            for k in range(pieces)
        ]
        for copy in copies:
            copy.start()
        wide = each * block
        stores = [
            pltpu.make_async_copy(
                out_ref.at[:, pl.ds(k * wide, wide)], out_hbm.at[:, pl.ds(k * wide, wide)], outs.at[k]
            )
            for k in range(pieces)
        ]
        got = jnp.concatenate([got_ref[g] for g in range(groups)], axis=0)
        fetched = dot_tn(chosen_ref[...], got)
        for c in range(comps):
            shells[:, c, :] = fetched[:, c * width : (c + 1) * width]
        for k in range(pieces):
            copies[k].wait()
            for b in range(k * each, (k + 1) * each):
                res = dot_nt(shells[b].astype(bf16), rbf_ref[b])
                out_ref[:, b * block : (b + 1) * block] = res[0:comps, :]
            stores[k].start()
        for copy in stores:
            copy.wait()

    return pl.pallas_call(
        kernel,
        out_shape=jax.ShapeDtypeStruct((comps, blocks * block), f32),
        in_specs=[spec(VMEM), spec(VMEM), spec(ANY)],
        out_specs=spec(ANY),
        scratch_shapes=[
            pltpu.VMEM((blocks, 8, width), f32),
            pltpu.VMEM(rbf.shape, bf16),
            pltpu.VMEM((comps, blocks * block), f32),
            pltpu.SemaphoreType.DMA((pieces,)),
            pltpu.SemaphoreType.DMA((pieces,)),
        ],
        name="wall",
        compiler_params=PARAMS,
    )(in_vmem(returned), in_vmem(chosen), in_hbm(rbf))


def per_device(
    flow,
    wall_motion,
    normal_operator,
    wall_coupling,
    wall_stencil,
    rbf_blocks,
    block_owner,
    block_row,
    displacement,
    stiffness,
    residual_history,
    solution_history,
):
    groups = lax.axis_size("fluid")
    devices = groups * lax.axis_size("solid")
    comps, points, normal = flow.shape
    blocks, block, width = rbf_blocks.shape
    count = residual_history.shape[0]
    rows = displacement.shape[0]
    capacity = max(2, (3 * blocks + 2 * groups - 1) // (2 * groups))
    slots = up_to(capacity + 1, 16)
    me = lax.axis_index(AXES).astype(jnp.int32).reshape(1)
    up = [(i, i + 1) for i in range(devices - 1)]
    down = [(i + 1, i) for i in range(devices - 1)]

    disp = displacement.transpose(1, 0, 2)
    res_hist = residual_history.transpose(0, 2, 1, 3).reshape(count, comps * rows, width)
    sol_hist = solution_history.transpose(0, 2, 1, 3).reshape(count, comps * rows, width)
    owner = block_owner.reshape(1, blocks)
    local_row = block_row.reshape(1, blocks)
    coupling = wall_coupling.reshape(1, normal)
    stencil = wall_stencil.reshape(1, normal)

    flow_tail = lax.ppermute(flow[:, points - 1 :, :], AXES, up)
    flow_head = lax.ppermute(flow[:, :1, :], AXES, down)
    gram, chosen, labels = gram_stage(owner, local_row, res_hist, groups, slots)
    tile = 1024 if points % 1024 == 0 else points
    new_flow, send = flow_stage(
        flow, flow_head, flow_tail, wall_motion, normal_operator, coupling, stencil, rbf_blocks, chosen, labels, gram,
        tile, slots, capacity,
    )
    arrived = lax.all_to_all(send, "fluid", 0, 0, tiled=True)
    force, gram, placed_labels, head, tail = place_stage(arrived, disp, stiffness, slots, capacity, count)
    before = lax.ppermute(tail, AXES, up)
    after = lax.ppermute(head, AXES, down)
    half = count // groups // 2
    solved, send = sweep_stage(me, force, disp, stiffness, before, after, res_hist, gram, half, devices)
    got = lax.all_to_all(send, AXES, 0, 0, tiled=True)
    fresh, reply, line = update_stage(got, sol_hist, solved, placed_labels, count, slots)
    returned = lax.all_to_all(reply, "fluid", 0, 0, tiled=True)
    wall_next = wall_stage(returned, chosen, rbf_blocks, comps)
    return (new_flow, fresh.transpose(1, 0, 2), wall_next, jnp.sqrt(line[0, count]))


def solution(mesh):
    return jax.shard_map(
        per_device,
        mesh=mesh,
        in_specs=(
            P(None, ("fluid", "solid"), None),
            P(None, ("fluid", "solid")),
            P(),
            P(),
            P(),
            P(("fluid", "solid"), None, None),
            P(("fluid", "solid"), None),
            P(("fluid", "solid"), None),
            P(("fluid", "solid"), None, None),
            P(("fluid", "solid"), None),
            P(None, ("fluid", "solid"), None, None),
            P(None, ("fluid", "solid"), None, None),
        ),
        out_specs=(
            P(None, ("fluid", "solid"), None),
            P(("fluid", "solid"), None, None),
            P(None, ("fluid", "solid")),
            P(),
        ),
        check_vma=False,
    )
```
